128 devices in a mesh: dp: 8 (over z_hi, x), seq: 16 (over z_lo, y, core).
Axes of the slice: x: 4, y: 4, z: 4 (z_hi: 2, z_lo: 2; z = z_hi * 2 + z_lo), core: 2. Of those that a mesh axis runs over, the one named last changes fastest.
Arguments:
- stream: bfloat16 [8, 512, 1536], P('dp', 'seq'), may hold values from -6 to 6
- queries: bfloat16 [8, 512, 1536], P('dp', 'seq'), may hold values from -30 to 30
- new_keys: bfloat16 [8, 512, 1536], P('dp', 'seq'), may hold values from -6.5 to 6.5
- new_values: bfloat16 [8, 512, 1536], P('dp', 'seq'), may hold values from -6 to 6
- cache_keys: bfloat16 [8, 1536, 1536], P('dp', 'seq'), may hold values from -6.375 to 6.375
- cache_values: bfloat16 [8, 1536, 1536], P('dp', 'seq'), may hold values from -6 to 6
- cache_frames: int32 [8, 1536], P('dp', 'seq'), may hold values from 0 to 20, as said below
- group_index: int32 [8], P('dp'), may hold values from 4 to 7, as said below
- timestep: int32 [8], P('dp'), may hold values from 0 to 3
- gate_table: float32 [4, 1536], replicated, may hold values from 0.1 to 1.9
- attn_out_weight: bfloat16 [1536, 1536], replicated, may hold values from -0.15625 to 0.15625
- critic_in: bfloat16 [131072, 1536], P(('dp', 'seq')), may hold values from -24 to 24
- critic_cot: bfloat16 [131072, 1536], P(('dp', 'seq')), may hold values from -6 to 6
- critic_weight: bfloat16 [1536, 1536], P(('dp', 'seq')), may hold values from -0.15625 to 0.15625
Outputs:
- stream_out: bfloat16 [8, 512, 1536], P('dp', 'seq')
- critic_grad_in: bfloat16 [131072, 1536], P(('dp', 'seq'))
- critic_grad_weight: float32 [1536, 1536], P(('dp', 'seq'))
The draws below stay inside these ranges and needn't reach their ends.
Inputs may be any that keep to these rules, and one draw needn't show every extreme that they name: `group_index`: index of the frame group; both ends are reached in every draw. `cache_frames`: sample b's cache holds the 12 frames 3 * group_index[b] - 12 to 3 * group_index[b] - 1, each in one contiguous run of slots, runs of equal length up to one slot, in a rotated order.
All inputs are finite; a program needn't handle non-finite values.
Results may differ from the reference program's by a relative error of at most 0.0045.
Values may be sent and summed in bfloat16 or wider, within the bound.
A program may use at most 128 MiB of HBM per device.

```python
import jax
import jax.numpy as jnp
from jax import lax

D = 1536
HEADS = 12
HEAD = 128
STEPS = 4
FRAMES_GROUP = 3
WINDOW_FRAMES = 9
BATCH = 8
GROUP = 512
CACHE = 1536
CRIT_ROWS = 131072


def drawn_pair(key):
    base = jax.random.fold_in(key, 4711)
    key_q, key_k = jax.random.split(base, 2)
    query_draw = jnp.clip(1.6 * jax.random.normal(key_q, (BATCH, GROUP, D), jnp.float32), -6.4, 6.4)
    key_draw = jnp.clip(1.6 * jax.random.normal(key_k, (BATCH, GROUP, D), jnp.float32), -6.4, 6.4)
    return (query_draw, key_draw)


def draw_queries(key, part):
    return drawn_pair(key)[0].astype(jnp.bfloat16)


def draw_new_keys(key, part):
    return drawn_pair(key)[1].astype(jnp.bfloat16)


def frame_layout(key):
    base = jax.random.fold_in(key, 9173)
    key_group, key_turn = jax.random.split(base, 2)
    cycle = FRAMES_GROUP + WINDOW_FRAMES
    group = jax.random.randint(key_group, (BATCH,), 4, 8, dtype=jnp.int32)
    group = group.at[0].set(7).at[BATCH - 1].set(4)
    turn = jax.random.randint(key_turn, (BATCH, 1), 0, cycle, dtype=jnp.int32)
    block = jnp.arange(CACHE, dtype=jnp.int32) * cycle // CACHE
    frames = FRAMES_GROUP * group[:, None] - cycle + (block[None, :] + turn) % cycle
    return (group, frames.astype(jnp.int32))


def draw_group_index(key, part):
    return frame_layout(key)[0]


def draw_cache_frames(key, part):
    return frame_layout(key)[1]


def plant(drawn, own_key, low, top_value):
    longest = drawn.shape.index(max(drawn.shape))
    spots = []
    for shift in (0, 1):
        where = [jax.random.randint(jax.random.fold_in(own_key, axis), (), 0, length) for axis, length in enumerate(drawn.shape)]
        where[longest] = (where[longest] + shift) % drawn.shape[longest]
        spots.append(tuple(where))
    return drawn.at[spots[0]].set(low).at[spots[1]].set(top_value)


def strengthened(entries, stream_key, source, target, parts, factor):
    def block_of(axis_at):
        return (jnp.arange(entries.shape[axis_at]) // (entries.shape[axis_at] // parts)).reshape((-1,) + (1,) * (entries.ndim - 1 - axis_at))

    one_side = jax.random.permutation(stream_key, parts)[block_of(target)]
    other_side = (block_of(target) + parts // 2) % parts
    return jnp.where((block_of(source) == one_side) | (block_of(source) == other_side), factor * entries, entries)


def shard_levels(key, shape, cuts, least, largest):
    def one(position, shards_of):
        heights = jax.random.uniform(jax.random.fold_in(jax.random.fold_in(key, 6), position), (shards_of,), jnp.float32, least / len(cuts), largest / len(cuts))
        return jnp.repeat(jnp.exp(heights), shape[position] // shards_of).reshape((-1,) + (1,) * (len(shape) - position - 1))

    loudness = one(*cuts[0])
    for cut in cuts[1:]:
        loudness = loudness * one(*cut)
    return loudness


def noise(key, shape, spread, limit, cuts=(), held_as=jnp.bfloat16):
    factor_of = shard_levels(key, shape, cuts, -0.22, 0.18) if cuts else 1.0
    values = jax.random.normal(key, shape, jnp.float32) * spread * factor_of
    return jnp.minimum(jnp.maximum(values, -limit), limit).astype(held_as)


def noise_with(key, shape, scale, bound, cuts, heavy, kind=jnp.bfloat16):
    array = scale * jax.random.normal(key, shape, jnp.float32)
    if cuts:
        array = array * shard_levels(key, shape, cuts, -0.22, 0.18)
    return jnp.clip(strengthened(array, jax.random.fold_in(key, 3), *heavy), -bound, bound).astype(kind)


def setup_inputs(seed: int = 0) -> dict:
    key_list = jax.random.split(jax.random.key(seed), 15)
    stream = noise(key_list[0], (BATCH, GROUP, D), 1.0, 6.0, ((0, 8), (1, 16)))
    queries = draw_queries(jax.random.fold_in(key_list[14], 71), 0)
    new_keys = draw_new_keys(jax.random.fold_in(key_list[14], 71), 0)
    new_values = noise(key_list[3], (BATCH, GROUP, D), 1.0, 6.0, ((0, 8), (1, 16)))
    cache_keys = noise(key_list[4], (BATCH, CACHE, D), 1.6, 6.375, ((0, 8), (1, 16)))
    cache_values = noise(key_list[5], (BATCH, CACHE, D), 1.0, 6.0, ((0, 8), (1, 16)))
    cache_frames = draw_cache_frames(jax.random.fold_in(key_list[14], 71), 0)
    group_index = draw_group_index(jax.random.fold_in(key_list[14], 71), 0)
    timestep = plant(jax.random.randint(key_list[8], (BATCH,), 0, STEPS), jax.random.fold_in(key_list[8], 1), 0, STEPS - 1).astype(jnp.int32)
    gate_table = jnp.clip(1.0 + 0.18 * jax.random.normal(key_list[9], (STEPS, D), jnp.float32), 0.1, 1.9)
    attn_out_weight = noise(key_list[10], (D, D), D ** -0.5, 0.15625)
    critic_in = noise_with(key_list[11], (CRIT_ROWS, D), 1.0, 24.0, ((0, 128),), (0, 1, 128, 5.5))
    critic_cot = noise(key_list[12], (CRIT_ROWS, D), 1.0, 6.0, ((0, 128),))
    critic_weight = noise(key_list[13], (D, D), D ** -0.5, 0.15625, ((0, 128),))
    return {"stream": stream, "queries": queries, "new_keys": new_keys, "new_values": new_values, "cache_keys": cache_keys, "cache_values": cache_values, "cache_frames": cache_frames, "group_index": group_index, "timestep": timestep, "gate_table": gate_table, "attn_out_weight": attn_out_weight, "critic_in": critic_in, "critic_cot": critic_cot, "critic_weight": critic_weight}


def attend_sample(packed):
    query_block, key_new, value_new, key_cache, value_cache, frames, group = packed
    keys = jnp.concatenate([key_cache, key_new], axis=0)
    values = jnp.concatenate([value_cache, value_new], axis=0)
    first = FRAMES_GROUP * group
    live_cache = (frames < first) & (frames >= first - WINDOW_FRAMES)
    live = jnp.concatenate([live_cache, jnp.ones((GROUP,), dtype=bool)])
    query_heads = query_block.reshape(GROUP, HEADS, HEAD).transpose(1, 0, 2)
    key_heads = keys.reshape(GROUP + CACHE, HEADS, HEAD).transpose(1, 0, 2)
    value_heads = values.reshape(GROUP + CACHE, HEADS, HEAD).transpose(1, 0, 2)

    def one_head(triple):
        q_head, k_head, v_head = triple
        scores = jnp.dot(q_head, k_head.T, preferred_element_type=jnp.float32) * (HEAD ** -0.5)
        scores = jnp.where(live[None, :], scores, -1e30)
        top = jnp.max(scores, axis=1, keepdims=True)
        weights = jnp.where(live[None, :], jnp.exp(scores - top), 0.0)
        totals = jnp.sum(weights, axis=1, keepdims=True)
        summed = jnp.dot(weights.astype(jnp.bfloat16), v_head, preferred_element_type=jnp.float32)
        return summed / totals

    mixed = lax.map(one_head, (query_heads, key_heads, value_heads))
    return mixed.transpose(1, 0, 2).reshape(GROUP, D).astype(jnp.bfloat16)


def reference(stream, queries, new_keys, new_values, cache_keys, cache_values, cache_frames, group_index, timestep, gate_table, attn_out_weight, critic_in, critic_cot, critic_weight):
    mixed = lax.map(attend_sample, (queries, new_keys, new_values, cache_keys, cache_values, cache_frames, group_index))
    projected = jnp.dot(mixed.reshape(BATCH * GROUP, D), attn_out_weight, preferred_element_type=jnp.float32).reshape(BATCH, GROUP, D)
    onehot = (timestep[:, None] == jnp.arange(STEPS, dtype=jnp.int32)[None, :]).astype(jnp.float32)
    gate = jnp.dot(onehot, gate_table, precision=lax.Precision.HIGHEST)
    stream_out = (stream.astype(jnp.float32) + gate[:, None, :] * projected).astype(jnp.bfloat16)
    grad_in = jnp.dot(critic_cot, critic_weight.T, preferred_element_type=jnp.float32).astype(jnp.bfloat16)
    grad_weight = jnp.dot(critic_in.T, critic_cot, preferred_element_type=jnp.float32) * (float(CRIT_ROWS) ** -0.5)
    return (stream_out, grad_in, grad_weight)
```

```python
import functools

import jax
import jax.numpy as jnp
from jax import lax
from jax.experimental import pallas as pl
from jax.experimental.pallas import tpu as pltpu
from jax.sharding import PartitionSpec as P

HEADS = 12
HEAD = 128
FRAMES_GROUP = 3
WINDOW_FRAMES = 9
D = 1536
HALF = 768
BF = jnp.bfloat16
F32 = jnp.float32
MESH = pl.DeviceIdType.MESH


def rem(a, n):
    return lax.rem(a, jnp.int32(n))


def div(a, n):
    return lax.div(a, jnp.int32(n))


def critic_kernel(
    cin_hbm, cot_hbm, wpad_hbm, gin_hbm, gw_ref,
    cin, cot, wown, tmp, wm, at, acc, dsend, drecv, rsend, rsend2,
    ra0, ra1, ra2, b0, b1, b2, b0s, b1s, b2s, rb0, rb1, rb2, c2, c2s, rc2, fsend, frecv, obuf,
    ld_sem, p0_s, p0_r, g1_s, g1_r, g2_s, g2_r, g3_s, g3_r, push_s, push_r,
    d_s, d_r, a_s, a_r, b_s, b_r, c_s, c_r, f_s, f_r, o_sem,
):
    dp = lax.axis_index("dp")
    seq = lax.axis_index("seq")
    zh, x = div(dp, 4), rem(dp, 4)
    zl, y, c = div(seq, 8), div(rem(seq, 8), 2), rem(seq, 2)
    z = zh * 2 + zl
    xh, xl = div(x, 2), rem(x, 2)
    plane = y * 2 + c
    partner = (dp, seq + 1 - 2 * c)

    def xdev(xx):
        return (zh * 4 + xx, seq)

    def zdev(zz):
        return (div(zz, 2) * 4 + x, rem(zz, 2) * 8 + plane)

    def ydev(yy, cc):
        return (dp, zl * 8 + yy * 2 + cc)

    def rcopy(src, dst, s_sem, r_sem, dev):
        return pltpu.make_async_remote_copy(
            src_ref=src, dst_ref=dst, send_sem=s_sem, recv_sem=r_sem, device_id=dev, device_id_type=MESH
        )

    loads = []
    for h in range(2):
        loads.append(pltpu.make_async_copy(cot_hbm.at[:, pl.ds(h * HALF, HALF)], cot.at[h], ld_sem.at[h]))
    for t in range(4):
        loads.append(pltpu.make_async_copy(cin_hbm.at[:, pl.ds(t * 384, 384)], cin.at[t], ld_sem.at[2 + t]))
    loads.append(pltpu.make_async_copy(wpad_hbm, wown, ld_sem.at[6]))
    loads[6].start()
    for ld in loads[:6]:
        ld.start()

    xs = [rem(x + s, 4) for s in (1, 2, 3)]
    ys = [rem(y + s, 4) for s in (1, 2, 3)]
    zs = [rem(z + s, 4) for s in (1, 2, 3)]
    plane_peers = [(rem(y + s, 4), c if k == 0 else 1 - c) for s in range(4) for k in range(2) if (s, k) != (0, 0)]

    barrier = pltpu.get_barrier_semaphore()
    peers = [xdev(v) for v in xs] + [zdev(v) for v in zs] + [ydev(a, b) for a, b in plane_peers]
    for dev in peers:
        pl.semaphore_signal(barrier, inc=1, device_id=dev, device_id_type=MESH)
    pl.semaphore_wait(barrier, len(peers))

    loads[6].wait()
    p0 = [
        rcopy(wown.at[b], tmp.at[plane], p0_s.at[k], p0_r.at[k], ydev(a, b))
        for k, (a, b) in enumerate(plane_peers)
    ]
    for cp in p0:
        cp.start()
    tmp[plane] = wown[c]

    def part2(ref, yy):
        return ref.at[..., pl.ds(pl.multiple_of(div(yy, 2) * 48, 48), 48), pl.ds(pl.multiple_of(512 + rem(yy, 2) * 128, 128), 128)]

    own = wm.at[c, zh, xh, xl, zl]
    g1 = []
    for k in range(3):
        g1.append(rcopy(own.at[:, pl.ds(0, 256)], own.at[:, pl.ds(0, 256)], g1_s.at[k], g1_r.at[k], xdev(xs[k])))
        g1.append(rcopy(own.at[:, pl.ds(256, 256)], own.at[:, pl.ds(256, 256)], g1_s.at[3 + k], g1_r.at[3 + k], zdev(zs[k])))
        g1.append(rcopy(part2(own, y), part2(own, y), g1_s.at[6 + k], g1_r.at[6 + k], xdev(xs[k])))
    g2 = []
    w0 = wm.at[c, zh, :, :, zl, :, pl.ds(0, 256)]
    w1 = wm.at[c, :, xh, xl, :, :, pl.ds(256, 256)]
    w2 = part2(wm.at[c, zh, :, :, zl], y)
    for k in range(3):
        g2.append(rcopy(w2, w2, g2_s.at[6 + k], g2_r.at[6 + k], zdev(zs[k])))
        g2.append(rcopy(w0, w0, g2_s.at[k], g2_r.at[k], zdev(zs[k])))
        g2.append(rcopy(w1, w1, g2_s.at[3 + k], g2_r.at[3 + k], xdev(xs[k])))
    w3 = part2(wm.at[c], y)
    g3 = [rcopy(w3, w3, g3_s.at[k], g3_r.at[k], ydev(ys[k], c)) for k in range(3)]

    for ld in loads[:6]:
        ld.wait()

    def dcopy(t):
        return rcopy(dsend.at[t], drecv.at[t], d_s.at[t], d_r.at[t], partner)

    @pl.loop(0, 4)
    def _(t):
        at[...] = cin[t].T
        dsend[t] = lax.dot_general(
            at[...], cot[1 - c], (((1,), (0,)), ((), ())), preferred_element_type=F32
        ).astype(BF)
        dcopy(t).start()
        acc[div(t, 2), rem(t, 2)] = lax.dot_general(
            at[...], cot[c], (((1,), (0,)), ((), ())), preferred_element_type=F32
        ).reshape(2, 2, 96, HALF)

        @pl.when(t == 0)
        def _():
            for cp in p0:
                cp.wait_recv()
            row = lax.broadcasted_iota(jnp.int32, (96, 128), 0)
            col = lax.broadcasted_iota(jnp.int32, (96, 128), 1)
            pick = (col == div(row, 12) * 16 + rem(row, 12)).astype(BF)
            block = jnp.dot(pick, tmp[...].reshape(128, HALF), preferred_element_type=F32).astype(BF)
            own[:, pl.ds(0, 512)] = block[:, :512]
            for yy in range(4):
                i, j = yy // 2 * 48, 512 + yy % 2 * 128

                @pl.when(y == yy)
                def _():
                    own[pl.ds(i, 48), pl.ds(j, 128)] = block[i : i + 48, j : j + 128]

            for cp in g1:
                cp.start()

        @pl.when(t == 1)
        def _():
            for cp in g1:
                cp.wait_recv()
            for cp in g2:
                cp.start()

        @pl.when(t == 2)
        def _():
            for cp in g2[0::3]:
                cp.wait_recv()
            for cp in g3:
                cp.start()

    @pl.loop(0, 4)
    def _(t):
        dcopy(t).wait_recv()
        i, j = div(t, 2), rem(t, 2)
        both = acc[i, j] + drecv[t].reshape(2, 2, 96, HALF).astype(F32)
        acc[i, j] = both
        rsend[i, j] = both[..., :512].astype(BF)
        for yy in range(4):
            rsend2[yy, i, j] = both[:, :, (yy // 2) * 48 : (yy // 2) * 48 + 48, 512 + (yy % 2) * 128 : 640 + (yy % 2) * 128].astype(BF)

    ra = []
    for k in range(3):
        ra.append(rcopy(rsend.at[div(zs[k], 2), :, :, rem(zs[k], 2), :, pl.ds(0, 256)], ra0.at[k], a_s.at[k], a_r.at[k], zdev(zs[k])))
        ra.append(rcopy(rsend.at[:, div(xs[k], 2), rem(xs[k], 2), :, :, pl.ds(256, 256)], ra1.at[k], a_s.at[3 + k], a_r.at[3 + k], xdev(xs[k])))
        ra.append(rcopy(rsend2.at[ys[k]], ra2.at[k], a_s.at[6 + k], a_r.at[6 + k], ydev(ys[k], c)))

    for cp in g2[1::3] + g2[2::3] + g3:
        cp.wait_recv()
    for cp in ra:
        cp.start()

    def pcopy(t):
        src = wm.at[c, div(t, 2), rem(t, 2)]
        return rcopy(src, src, push_s.at[t], push_r.at[t], partner)

    for t in range(4):
        pcopy(jnp.int32(t)).start()

    def ocopy(t):
        return pltpu.make_async_copy(obuf.at[t], gin_hbm.at[:, pl.ds(pl.multiple_of(t * 384, 384), 384)], o_sem.at[t])

    @pl.loop(0, 4)
    def _(t):
        pcopy(t).wait_recv()
        i, j = div(t, 2), rem(t, 2)
        dims = (((1,), (1,)), ((), ()))
        res = lax.dot_general(cot[0], wm[0, i, j].reshape(384, HALF), dims, preferred_element_type=F32)
        res = res + lax.dot_general(cot[1], wm[1, i, j].reshape(384, HALF), dims, preferred_element_type=F32)
        obuf[t] = res.astype(BF)
        ocopy(t).start()

    for cp in ra:
        cp.wait_recv()
    v0 = acc[zh, :, :, zl, :, 0:256]
    v1 = acc[:, xh, xl, :, :, 256:512]
    for k in range(3):
        v0 = v0 + ra0[k].astype(F32)
        v1 = v1 + ra1[k].astype(F32)
    b0[...] = v0
    b1[...] = v1
    b0s[...] = v0.astype(BF)
    b1s[...] = v1.astype(BF)
    v2 = rsend2[y].astype(F32)
    for k in range(3):
        v2 = v2 + ra2[k].astype(F32)
    b2[...] = v2
    b2s[...] = v2.astype(BF)

    rb = []
    for k in range(3):
        rb.append(rcopy(b2s.at[div(zs[k], 2), :, :, rem(zs[k], 2)], rb2.at[k], b_s.at[6 + k], b_r.at[6 + k], zdev(zs[k])))
        rb.append(rcopy(b0s.at[div(xs[k], 2), rem(xs[k], 2)], rb0.at[k], b_s.at[k], b_r.at[k], xdev(xs[k])))
        rb.append(rcopy(b1s.at[div(zs[k], 2), rem(zs[k], 2)], rb1.at[k], b_s.at[3 + k], b_r.at[3 + k], zdev(zs[k])))
    for cp in rb:
        cp.start()
    for cp in rb[0::3]:
        cp.wait_recv()
    v2 = b2[zh, :, :, zl]
    for k in range(3):
        v2 = v2 + rb2[k].astype(F32)
    c2[...] = v2
    c2s[...] = v2.astype(BF)
    rc = [rcopy(c2s.at[div(xs[k], 2), rem(xs[k], 2)], rc2.at[k], c_s.at[k], c_r.at[k], xdev(xs[k])) for k in range(3)]
    for cp in rc:
        cp.start()
    for cp in rb[1::3] + rb[2::3]:
        cp.wait_recv()
    r0 = b0[xh, xl]
    r1 = b1[zh, zl]
    for k in range(3):
        r0 = r0 + rb0[k].astype(F32)
        r1 = r1 + rb1[k].astype(F32)
    for cp in rc:
        cp.wait_recv()
    r2 = c2[xh, xl]
    for k in range(3):
        r2 = r2 + rc2[k].astype(F32)

    row = lax.broadcasted_iota(jnp.int32, (96, 256), 0)
    col = lax.broadcasted_iota(jnp.int32, (96, 256), 1)
    mine = (div(row, 48) == div(y, 2)) & (div(col, 128) == rem(y, 2))
    r2 = jnp.concatenate([r2, r2], axis=0)
    r2 = jnp.where(mine, jnp.concatenate([r2, r2], axis=1), 0.0)
    row = lax.broadcasted_iota(jnp.int32, (128, 96), 0)
    col = lax.broadcasted_iota(jnp.int32, (128, 96), 1)
    place = ((col == div(row, 16) * 12 + rem(row, 16)) & (rem(row, 16) < 12)).astype(BF)
    full = jnp.concatenate([r0, r1, r2], axis=1).astype(BF)
    fsend[...] = jnp.dot(place, full, preferred_element_type=F32).astype(BF).reshape(8, 16, HALF)
    fin = [
        rcopy(fsend.at[a * 2 + b], frecv.at[plane], f_s.at[k], f_r.at[k], ydev(a, b))
        for k, (a, b) in enumerate(plane_peers)
    ]
    for cp in fin:
        cp.start()
    frecv[plane] = fsend[plane]
    for cp in fin:
        cp.wait_recv()
    factor = float(131072) ** (-0.5)
    for h in range(2):
        total = frecv[h].astype(F32)
        for yy in range(1, 4):
            total = total + frecv[yy * 2 + h].astype(F32)
        gw_ref[:, pl.ds(h * HALF, HALF)] = total[:12] * factor

    for cp in p0 + g1 + g2 + g3 + ra + rb + rc + fin:
        cp.wait_send()
    for t in range(4):
        dcopy(jnp.int32(t)).wait_send()
        pcopy(jnp.int32(t)).wait_send()
        ocopy(jnp.int32(t)).wait()


def critic_pass(critic_in, critic_cot, critic_weight):
    wpad = jnp.pad(critic_weight, ((0, 4), (0, 0))).reshape(16, 2, HALF).transpose(1, 0, 2)
    dma = pltpu.SemaphoreType.DMA
    V = pltpu.VMEM
    any_spec = pl.BlockSpec(memory_space=pl.ANY)
    return pl.pallas_call(
        critic_kernel,
        out_shape=(
            jax.ShapeDtypeStruct((1024, D), BF),
            jax.ShapeDtypeStruct((12, D), F32),
        ),
        in_specs=[any_spec] * 3,
        out_specs=(any_spec, pl.BlockSpec(memory_space=pltpu.VMEM)),
        scratch_shapes=[
            V((4, 1024, 384), BF), V((2, 1024, HALF), BF), V((2, 16, HALF), BF), V((8, 16, HALF), BF),
            V((2, 2, 2, 2, 2, 96, HALF), BF), V((384, 1024), BF), V((2, 2, 2, 2, 96, HALF), F32),
            V((4, 384, HALF), BF), V((4, 384, HALF), BF),
            V((2, 2, 2, 2, 96, 512), BF), V((4, 2, 2, 2, 2, 48, 128), BF),
            V((3, 2, 2, 96, 256), BF), V((3, 2, 2, 96, 256), BF), V((3, 2, 2, 2, 2, 48, 128), BF),
            V((2, 2, 96, 256), F32), V((2, 2, 96, 256), F32), V((2, 2, 2, 2, 48, 128), F32),
            V((2, 2, 96, 256), BF), V((2, 2, 96, 256), BF), V((2, 2, 2, 2, 48, 128), BF),
            V((3, 96, 256), BF), V((3, 96, 256), BF), V((3, 2, 2, 48, 128), BF),
            V((2, 2, 48, 128), F32), V((2, 2, 48, 128), BF), V((3, 48, 128), BF),
            V((8, 16, HALF), BF), V((8, 16, HALF), BF), V((4, 1024, 384), BF),
            dma((7,)), dma((7,)), dma((7,)), dma((9,)), dma((9,)), dma((9,)), dma((9,)), dma((3,)), dma((3,)),
            dma((4,)), dma((4,)), dma((4,)), dma((4,)), dma((9,)), dma((9,)), dma((9,)), dma((9,)),
            dma((3,)), dma((3,)), dma((7,)), dma((7,)), dma((4,)),
        ],
        compiler_params=pltpu.CompilerParams(
            collective_id=0, has_side_effects=True, vmem_limit_bytes=60 * 1024 * 1024
        ),
        cost_estimate=pl.CostEstimate(flops=9663676416, bytes_accessed=20000000, transcendentals=0),
    )(critic_in, critic_cot, wpad)


def attention(stream, queries, new_keys, new_values, cache_keys, cache_values, cache_frames, group_index, timestep, gate_table, attn_out_weight):
    first_frame = FRAMES_GROUP * group_index[0]
    frames = cache_frames[0]
    live_cache = (frames < first_frame) & (frames >= first_frame - WINDOW_FRAMES)
    live = jnp.concatenate([live_cache, jnp.ones((32,), dtype=bool)]).astype(BF)
    live = jnp.broadcast_to(live[None, :], (16, HEAD))
    live = jnp.broadcast_to(live[:, None, :], (16, HEADS, HEAD))
    rows = jnp.concatenate(
        [a.reshape(-1, HEADS, HEAD) for a in (cache_keys[0], new_keys[0], cache_values[0], new_values[0], queries[0])] + [live],
        axis=0,
    ).transpose(1, 0, 2)
    rows = jnp.pad(rows, ((0, 4), (0, 0), (0, 0)))
    got = lax.all_to_all(rows, "seq", 0, 0, tiled=True)
    keys = got[:, 0:128].reshape(2048, HEAD)
    values = got[:, 128:256].reshape(2048, HEAD)
    q = got[:, 256:288].reshape(512, HEAD)
    alive = got[:, 288, :].reshape(1, 2048) > 0
    scores = lax.dot_general(q, keys, (((1,), (1,)), ((), ())), preferred_element_type=F32) * (HEAD ** (-0.5))
    scores = jnp.where(alive, scores, -1e30)
    top = jnp.max(scores, axis=1, keepdims=True)
    weights = jnp.where(alive, jnp.exp(scores - top), 0.0)
    totals = jnp.sum(weights, axis=1, keepdims=True)
    summed = jnp.dot(weights.astype(BF), values, preferred_element_type=F32)
    mixed = (summed / totals).astype(BF).reshape(16, 32, HEAD)
    back = lax.all_to_all(mixed, "seq", 0, 0, tiled=True)
    mixed = back[:HEADS].transpose(1, 0, 2).reshape(32, D)
    projected = jnp.dot(mixed, attn_out_weight, preferred_element_type=F32)
    onehot = (timestep[:, None] == jnp.arange(gate_table.shape[0], dtype=jnp.int32)[None, :]).astype(F32)
    gate = jnp.dot(onehot, gate_table, precision=lax.Precision.HIGHEST)
    return (stream[0].astype(F32) + gate * projected).astype(BF)[None]


def local(*args):
    stream_out = attention(*args[:11])
    grad_in, grad_weight = critic_pass(*args[11:])
    return (stream_out, grad_in, grad_weight)


def solution(mesh):
    three = P("dp", "seq", None)
    rows = P(("dp", "seq"), None)
    return jax.shard_map(
        local,
        mesh=mesh,
        in_specs=(three,) * 6 + (P("dp", "seq"), P("dp"), P("dp"), P(), P(), rows, rows, rows),
        out_specs=(three, rows, rows),
        check_vma=False,
    )
```

```python
import functools

import jax
import jax.numpy as jnp
from jax import lax
from jax.experimental import pallas as pl
from jax.experimental.pallas import tpu as pltpu
from jax.sharding import PartitionSpec as P

HEADS = 12
HEAD = 128
FRAMES_GROUP = 3
WINDOW_FRAMES = 9
D = 1536
HALF = 768
BF = jnp.bfloat16
F32 = jnp.float32
MESH = pl.DeviceIdType.MESH


def rem(a, n):
    return lax.rem(a, jnp.int32(n))


def div(a, n):
    return lax.div(a, jnp.int32(n))


SCOPE = [None]


def sc(name=None):
    if SCOPE[0] is not None:
        SCOPE[0].__exit__(None, None, None)
    SCOPE[0] = None
    if name and PROFILE:
        SCOPE[0] = jax.named_scope(name)
        SCOPE[0].__enter__()


PROFILE = False


def owner(h):
    u, r = h // 3, h % 3
    zl = u // 2
    y = (u % 2) * 2 + (zl if r < 2 else 1 - zl)
    return zl * 8 + y * 2 + (r if r < 2 else 1)


def fused_kernel(
    stream_ref, q_hbm, nk_hbm, nv_hbm, ck_hbm, cv_hbm, frames_ref, group_ref, step_ref, gate_ref, aow_hbm,
    cin_hbm, cot_hbm, w_ref, so_ref, gin_hbm, gw_ref,
    kbuf, vbuf, qbuf, aow, msg, got, ob, mixed,
    cin, cot, wown, tmp, wm, at, acc, dsend, drecv, rsend, rsend2,
    ra0, ra1, ra2, b0, b1, b2, b0s, b1s, b2s, rb0, rb1, rb2, c2, c2s, rc2, fsend, frecv, obuf,
    ld_sem, p0_s, p0_r, g1_s, g1_r, g2_s, g2_r, g3_s, g3_r, push_s, push_r,
    d_s, d_r, a_s, a_r, b_s, b_r, c_s, c_r, f_s, f_r, o_sem, m_s, m_r, o_s, o_r,
):
    dp = lax.axis_index("dp")
    seq = lax.axis_index("seq")
    zh, x = div(dp, 4), rem(dp, 4)
    zl, y, c = div(seq, 8), div(rem(seq, 8), 2), rem(seq, 2)
    z = zh * 2 + zl
    xh, xl = div(x, 2), rem(x, 2)
    plane = y * 2 + c
    partner = (dp, seq + 1 - 2 * c)

    def xdev(xx):
        return (zh * 4 + xx, seq)

    def zdev(zz):
        return (div(zz, 2) * 4 + x, rem(zz, 2) * 8 + plane)

    def ydev(yy, cc):
        return (dp, zl * 8 + yy * 2 + cc)

    def rcopy(src, dst, s_sem, r_sem, dev):
        return pltpu.make_async_remote_copy(
            src_ref=src, dst_ref=dst, send_sem=s_sem, recv_sem=r_sem, device_id=dev, device_id_type=MESH
        )

    pairs = [(q_hbm, qbuf), (ck_hbm, kbuf.at[pl.ds(0, 96)]), (nk_hbm, kbuf.at[pl.ds(96, 32)]),
             (cv_hbm, vbuf.at[pl.ds(0, 96)]), (nv_hbm, vbuf.at[pl.ds(96, 32)])]
    pairs += [(cot_hbm.at[:, pl.ds(h * HALF, HALF)], cot.at[h]) for h in range(2)]
    pairs += [(cin_hbm.at[:, pl.ds(t * 384, 384)], cin.at[t]) for t in range(4)]
    pairs += [(aow_hbm, aow)]
    loads = [pltpu.make_async_copy(a, b, ld_sem.at[k]) for k, (a, b) in enumerate(pairs)]
    for ld in loads:
        ld.start()

    xs = [rem(x + s, 4) for s in (1, 2, 3)]
    ys = [rem(y + s, 4) for s in (1, 2, 3)]
    zs = [rem(z + s, 4) for s in (1, 2, 3)]
    plane_peers = [(rem(y + s, 4), c if k == 0 else 1 - c) for s in range(4) for k in range(2) if (s, k) != (0, 0)]
    others = [rem(seq + s, 16) for s in range(1, 16)]

    sc("barrier")
    barrier = pltpu.get_barrier_semaphore()
    peers = [xdev(v) for v in xs] + [((1 - zh) * 4 + x, v * 8 + plane) for v in range(2)] + [(dp, v) for v in others]
    for dev in peers:
        pl.semaphore_signal(barrier, inc=1, device_id=dev, device_id_type=MESH)
    for h in range(2):
        wown[h] = jnp.zeros((16, HALF), BF)
        wown[h, pl.ds(0, 12), :] = w_ref[:, pl.ds(h * HALF, HALF)]
    pl.semaphore_wait(barrier, len(peers))

    p0 = [
        rcopy(wown.at[b], tmp.at[plane], p0_s.at[k], p0_r.at[k], ydev(a, b))
        for k, (a, b) in enumerate(plane_peers)
    ]
    for cp in p0:
        cp.start()
    tmp[plane] = wown[c]

    sc("msg")
    for ld in loads[:5]:
        ld.wait()
    first = FRAMES_GROUP * group_ref[0]
    frames = frames_ref[...]
    live = jnp.where((frames < first) & (frames >= first - WINDOW_FRAMES), 1.0, 0.0)
    live = jnp.broadcast_to(live, (16, 96)).astype(BF)
    for h in range(HEADS):
        cols = pl.ds(h * HEAD, HEAD)
        msg[h, pl.ds(0, 128), :] = kbuf[:, cols]
        msg[h, pl.ds(128, 128), :] = vbuf[:, cols]
        msg[h, pl.ds(256, 32), :] = qbuf[:, cols]
        msg[h, pl.ds(288, 16), :] = jnp.ones((16, HEAD), BF)
        msg[h, pl.ds(288, 16), pl.ds(0, 96)] = live

    def mcopy(h):
        return rcopy(msg.at[h], got.at[seq], m_s.at[h], m_r.at[seq], (dp, owner(h)))

    def part2(ref, yy):
        return ref.at[..., pl.ds(pl.multiple_of(div(yy, 2) * 48, 48), 48), pl.ds(pl.multiple_of(512 + rem(yy, 2) * 128, 128), 128)]

    own = wm.at[c, zh, xh, xl, zl]
    g1 = []
    for k in range(3):
        g1.append(rcopy(own.at[:, pl.ds(0, 256)], own.at[:, pl.ds(0, 256)], g1_s.at[k], g1_r.at[k], xdev(xs[k])))
        g1.append(rcopy(own.at[:, pl.ds(256, 256)], own.at[:, pl.ds(256, 256)], g1_s.at[3 + k], g1_r.at[3 + k], zdev(zs[k])))
        g1.append(rcopy(part2(own, y), part2(own, y), g1_s.at[6 + k], g1_r.at[6 + k], xdev(xs[k])))
    g2 = []
    w0 = wm.at[c, zh, :, :, zl, :, pl.ds(0, 256)]
    w1 = wm.at[c, :, xh, xl, :, :, pl.ds(256, 256)]
    w2 = part2(wm.at[c, zh, :, :, zl], y)
    for k in range(3):
        g2.append(rcopy(w2, w2, g2_s.at[6 + k], g2_r.at[6 + k], zdev(zs[k])))
        g2.append(rcopy(w0, w0, g2_s.at[k], g2_r.at[k], zdev(zs[k])))
        g2.append(rcopy(w1, w1, g2_s.at[3 + k], g2_r.at[3 + k], xdev(xs[k])))
    w3 = part2(wm.at[c], y)
    g3 = [rcopy(w3, w3, g3_s.at[k], g3_r.at[k], ydev(ys[k], c)) for k in range(3)]

    sc("ldwait")
    for ld in loads[5:11]:
        ld.wait()
    sc()

    def dcopy(t):
        return rcopy(dsend.at[t], drecv.at[t], d_s.at[t], d_r.at[t], partner)

    @pl.loop(0, 4)
    def _(t):
        sc("gw")
        at[...] = cin[t].T
        dsend[t] = lax.dot_general(
            at[...], cot[1 - c], (((1,), (0,)), ((), ())), preferred_element_type=F32
        ).astype(BF)
        dcopy(t).start()
        acc[div(t, 2), rem(t, 2)] = lax.dot_general(
            at[...], cot[c], (((1,), (0,)), ((), ())), preferred_element_type=F32
        ).reshape(2, 2, 96, HALF)
        sc("comm0")

        @pl.when(t == 0)
        def _():
            for cp in p0:
                cp.wait_recv()
            row = lax.broadcasted_iota(jnp.int32, (96, 128), 0)
            col = lax.broadcasted_iota(jnp.int32, (96, 128), 1)
            pick = (col == div(row, 12) * 16 + rem(row, 12)).astype(BF)
            block = jnp.dot(pick, tmp[...].reshape(128, HALF), preferred_element_type=F32).astype(BF)
            own[:, pl.ds(0, 512)] = block[:, :512]
            for yy in range(4):
                i, j = yy // 2 * 48, 512 + yy % 2 * 128

                @pl.when(y == yy)
                def _():
                    own[pl.ds(i, 48), pl.ds(j, 128)] = block[i : i + 48, j : j + 128]

            for cp in g1:
                cp.start()

        sc("comm1")

        @pl.when(t == 1)
        def _():
            for cp in g1:
                cp.wait_recv()
            for cp in g2:
                cp.start()
            for h in range(HEADS):

                @pl.when(seq != owner(h))
                def _():
                    mcopy(h).start()

                @pl.when(seq == owner(h))
                def _():
                    got[seq] = msg[h]

        sc()

    @pl.loop(0, 4)
    def _(t):
        sc("dwait")
        dcopy(t).wait_recv()
        sc("chipsum")
        i, j = div(t, 2), rem(t, 2)
        both = acc[i, j] + drecv[t].reshape(2, 2, 96, HALF).astype(F32)
        acc[i, j] = both
        rsend[i, j] = both[..., :512].astype(BF)
        for yy in range(4):
            rsend2[yy, i, j] = both[:, :, (yy // 2) * 48 : (yy // 2) * 48 + 48, 512 + (yy % 2) * 128 : 640 + (yy % 2) * 128].astype(BF)
        sc()

    sc("rastart")
    ra = []
    for k in range(3):
        ra.append(rcopy(rsend.at[div(zs[k], 2), :, :, rem(zs[k], 2), :, pl.ds(0, 256)], ra0.at[k], a_s.at[k], a_r.at[k], zdev(zs[k])))
        ra.append(rcopy(rsend.at[:, div(xs[k], 2), rem(xs[k], 2), :, :, pl.ds(256, 256)], ra1.at[k], a_s.at[3 + k], a_r.at[3 + k], xdev(xs[k])))
        ra.append(rcopy(rsend2.at[ys[k]], ra2.at[k], a_s.at[6 + k], a_r.at[6 + k], ydev(ys[k], c)))
    for cp in ra:
        cp.start()

    sc("g2wait")
    for cp in g2[0::3]:
        cp.wait_recv()
    for cp in g3:
        cp.start()
    sc("g2wait2")
    for cp in g2[1::3] + g2[2::3]:
        cp.wait_recv()

    def pcopy(k, t):
        src = wm.at[c, div(t, 2), rem(t, 2), :, :, :, pl.ds(512 * k, 512 - 256 * k)]
        return rcopy(src, src, push_s.at[4 * k + t], push_r.at[4 * k + t], partner)

    for t in range(4):
        pcopy(0, jnp.int32(t)).start()

    double = rem(y, 2) == zl
    active = double | (c == 1)
    head = 3 * (zl * 2 + div(y, 2)) + jnp.where(double, c, 2)

    def mixcopy(k):
        return rcopy(ob.at[others[k]], mixed.at[head], o_s.at[k], o_r.at[head], (dp, others[k]))

    sc("attwait")

    @pl.when(active)
    def _():
        for src in others:
            rcopy(msg.at[0], got.at[src], m_s.at[0], m_r.at[src], partner).wait_recv()

    sc("att")

    @pl.when(active)
    def _():
        alive = jnp.concatenate([got[j, pl.ds(288, 16), :] for j in range(16)], axis=1)[0:1].astype(F32) > 0.5

        @pl.loop(0, 4)
        def _(i):
            q = got[pl.ds(i * 4, 4), pl.ds(256, 32), :].reshape(128, HEAD)
            keys = got[:, pl.ds(0, 128), :].reshape(2048, HEAD)
            values = got[:, pl.ds(128, 128), :].reshape(2048, HEAD)
            scores = lax.dot_general(q, keys, (((1,), (1,)), ((), ())), preferred_element_type=F32) * (HEAD ** (-0.5))
            scores = jnp.where(alive, scores, -1e30)
            top = jnp.max(scores, axis=1, keepdims=True)
            weights = jnp.where(alive, jnp.exp(scores - top), 0.0)
            totals = jnp.sum(weights, axis=1, keepdims=True)
            summed = jnp.dot(weights.astype(BF), values, preferred_element_type=F32)
            ob[pl.ds(i * 4, 4)] = (summed / totals).astype(BF).reshape(4, 32, HEAD)

        for k in range(15):
            mixcopy(k).start()
        mixed[head] = ob[seq]

    sc("g3wait")
    for cp in g3:
        cp.wait_recv()
    for t in range(4):
        pcopy(1, jnp.int32(t)).start()
    sc()

    def ocopy(t):
        return pltpu.make_async_copy(obuf.at[t], gin_hbm.at[:, pl.ds(pl.multiple_of(t * 384, 384), 384)], o_sem.at[t])

    rb = []
    for k in range(3):
        rb.append(rcopy(b2s.at[div(zs[k], 2), :, :, rem(zs[k], 2)], rb2.at[k], b_s.at[6 + k], b_r.at[6 + k], zdev(zs[k])))
        rb.append(rcopy(b0s.at[div(xs[k], 2), rem(xs[k], 2)], rb0.at[k], b_s.at[k], b_r.at[k], xdev(xs[k])))
        rb.append(rcopy(b1s.at[div(zs[k], 2), rem(zs[k], 2)], rb1.at[k], b_s.at[3 + k], b_r.at[3 + k], zdev(zs[k])))
    rc = [rcopy(c2s.at[div(xs[k], 2), rem(xs[k], 2)], rc2.at[k], c_s.at[k], c_r.at[k], xdev(xs[k])) for k in range(3)]

    @pl.loop(0, 4)
    def _(t):
        sc("pwait")
        pcopy(0, t).wait_recv()
        pcopy(1, t).wait_recv()
        sc("gin")
        i, j = div(t, 2), rem(t, 2)
        dims = (((1,), (1,)), ((), ()))
        res = lax.dot_general(cot[0], wm[0, i, j].reshape(384, HALF), dims, preferred_element_type=F32)
        res = res + lax.dot_general(cot[1], wm[1, i, j].reshape(384, HALF), dims, preferred_element_type=F32)
        obuf[t] = res.astype(BF)
        ocopy(t).start()

        sc("rawait")

        @pl.when(t == 0)
        def _():
            for cp in ra:
                cp.wait_recv()
            v0 = acc[zh, :, :, zl, :, 0:256]
            v1 = acc[:, xh, xl, :, :, 256:512]
            for k in range(3):
                v0 = v0 + ra0[k].astype(F32)
                v1 = v1 + ra1[k].astype(F32)
            b0[...] = v0
            b1[...] = v1
            b0s[...] = v0.astype(BF)
            b1s[...] = v1.astype(BF)
            v2 = rsend2[y].astype(F32)
            for k in range(3):
                v2 = v2 + ra2[k].astype(F32)
            b2[...] = v2
            b2s[...] = v2.astype(BF)
            for cp in rb:
                cp.start()

        sc("rbwait")

        @pl.when(t == 2)
        def _():
            for cp in rb[0::3]:
                cp.wait_recv()
            v2 = b2[zh, :, :, zl]
            for k in range(3):
                v2 = v2 + rb2[k].astype(F32)
            c2[...] = v2
            c2s[...] = v2.astype(BF)
            for cp in rc:
                cp.start()

        sc()

    sc("rbwait2")
    for cp in rb[1::3] + rb[2::3]:
        cp.wait_recv()
    r0 = b0[xh, xl]
    r1 = b1[zh, zl]
    for k in range(3):
        r0 = r0 + rb0[k].astype(F32)
        r1 = r1 + rb1[k].astype(F32)
    sc("rcwait")
    for cp in rc:
        cp.wait_recv()
    sc("last")
    r2 = c2[xh, xl]
    for k in range(3):
        r2 = r2 + rc2[k].astype(F32)

    row = lax.broadcasted_iota(jnp.int32, (96, 256), 0)
    col = lax.broadcasted_iota(jnp.int32, (96, 256), 1)
    mine = (div(row, 48) == div(y, 2)) & (div(col, 128) == rem(y, 2))
    r2 = jnp.concatenate([r2, r2], axis=0)
    r2 = jnp.where(mine, jnp.concatenate([r2, r2], axis=1), 0.0)
    row = lax.broadcasted_iota(jnp.int32, (128, 96), 0)
    col = lax.broadcasted_iota(jnp.int32, (128, 96), 1)
    place = ((col == div(row, 16) * 12 + rem(row, 16)) & (rem(row, 16) < 12)).astype(BF)
    full = jnp.concatenate([r0, r1, r2], axis=1).astype(BF)
    fsend[...] = jnp.dot(place, full, preferred_element_type=F32).astype(BF).reshape(8, 16, HALF)
    fin = [
        rcopy(fsend.at[a * 2 + b], frecv.at[plane], f_s.at[k], f_r.at[k], ydev(a, b))
        for k, (a, b) in enumerate(plane_peers)
    ]
    for cp in fin:
        cp.start()
    frecv[plane] = fsend[plane]

    sc("mixwait")
    for h in range(HEADS):

        @pl.when(seq != owner(h))
        def _():
            rcopy(ob.at[0], mixed.at[h], o_s.at[0], o_r.at[h], partner).wait_recv()

    loads[11].wait()
    sc("proj")
    joined = jnp.concatenate([mixed[h] for h in range(HEADS)], axis=1)
    projected = jnp.dot(joined, aow[...], preferred_element_type=F32)
    row = lax.broadcasted_iota(jnp.int32, (4, D), 0)
    gate = jnp.sum(jnp.where(row == step_ref[0], gate_ref[...], 0.0), axis=0, keepdims=True)
    so_ref[...] = (stream_ref[...].astype(F32) + gate * projected).astype(BF)

    sc("finwait")
    for cp in fin:
        cp.wait_recv()
    sc("drain")
    factor = float(131072) ** (-0.5)
    for h in range(2):
        total = frecv[h].astype(F32)
        for yy in range(1, 4):
            total = total + frecv[yy * 2 + h].astype(F32)
        gw_ref[:, pl.ds(h * HALF, HALF)] = total[:12] * factor

    for cp in p0 + g1 + g2 + g3 + ra + rb + rc + fin:
        cp.wait_send()
    for t in range(4):
        dcopy(jnp.int32(t)).wait_send()
        pcopy(0, jnp.int32(t)).wait_send()
        pcopy(1, jnp.int32(t)).wait_send()
        ocopy(jnp.int32(t)).wait()
    for h in range(HEADS):

        @pl.when(seq != owner(h))
        def _():
            mcopy(h).wait_send()

    @pl.when(active)
    def _():
        for k in range(15):
            mixcopy(k).wait_send()

    sc()


def local(stream, queries, new_keys, new_values, cache_keys, cache_values, cache_frames, group_index, timestep, gate_table, attn_out_weight, critic_in, critic_cot, critic_weight):
    dma = pltpu.SemaphoreType.DMA
    V = pltpu.VMEM
    anywhere = pl.BlockSpec(memory_space=pl.ANY)
    vmem = pl.BlockSpec(memory_space=pltpu.VMEM)
    smem = pl.BlockSpec(memory_space=pltpu.SMEM)
    so, gin, gw = pl.pallas_call(
        fused_kernel,
        out_shape=(
            jax.ShapeDtypeStruct((32, D), BF),
            jax.ShapeDtypeStruct((1024, D), BF),
            jax.ShapeDtypeStruct((12, D), F32),
        ),
        in_specs=[vmem] + [anywhere] * 5 + [vmem, smem, smem, vmem] + [anywhere] * 3 + [vmem],
        out_specs=(vmem, anywhere, vmem),
        scratch_shapes=[
            V((128, D), BF), V((128, D), BF), V((32, D), BF), V((D, D), BF), V((HEADS, 304, HEAD), BF),
            V((16, 304, HEAD), BF), V((16, 32, HEAD), BF), V((HEADS, 32, HEAD), BF),
            V((4, 1024, 384), BF), V((2, 1024, HALF), BF), V((2, 16, HALF), BF), V((8, 16, HALF), BF),
            V((2, 2, 2, 2, 2, 96, HALF), BF), V((384, 1024), BF), V((2, 2, 2, 2, 96, HALF), F32),
            V((4, 384, HALF), BF), V((4, 384, HALF), BF),
            V((2, 2, 2, 2, 96, 512), BF), V((4, 2, 2, 2, 2, 48, 128), BF),
            V((3, 2, 2, 96, 256), BF), V((3, 2, 2, 96, 256), BF), V((3, 2, 2, 2, 2, 48, 128), BF),
            V((2, 2, 96, 256), F32), V((2, 2, 96, 256), F32), V((2, 2, 2, 2, 48, 128), F32),
            V((2, 2, 96, 256), BF), V((2, 2, 96, 256), BF), V((2, 2, 2, 2, 48, 128), BF),
            V((3, 96, 256), BF), V((3, 96, 256), BF), V((3, 2, 2, 48, 128), BF),
            V((2, 2, 48, 128), F32), V((2, 2, 48, 128), BF), V((3, 48, 128), BF),
            V((8, 16, HALF), BF), V((8, 16, HALF), BF), V((4, 1024, 384), BF),
            dma((12,)), dma((7,)), dma((7,)), dma((9,)), dma((9,)), dma((9,)), dma((9,)), dma((3,)), dma((3,)),
            dma((8,)), dma((8,)), dma((4,)), dma((4,)), dma((9,)), dma((9,)), dma((9,)), dma((9,)),
            dma((3,)), dma((3,)), dma((7,)), dma((7,)), dma((4,)), dma((12,)), dma((16,)), dma((15,)), dma((12,)),
        ],
        compiler_params=pltpu.CompilerParams(
            collective_id=0, has_side_effects=True, vmem_limit_bytes=60 * 1024 * 1024
        ),
        cost_estimate=pl.CostEstimate(flops=10500000000, bytes_accessed=25000000, transcendentals=1000000),
    )(
        stream[0], queries[0], new_keys[0], new_values[0], cache_keys[0], cache_values[0], cache_frames,
        group_index, timestep, gate_table, attn_out_weight, critic_in, critic_cot, critic_weight,
    )
    return (so[None], gin, gw)


def solution(mesh):
    three = P("dp", "seq", None)
    rows = P(("dp", "seq"), None)
    return jax.shard_map(
        local,
        mesh=mesh,
        in_specs=(three,) * 6 + (P("dp", "seq"), P("dp"), P("dp"), P(), P(), rows, rows, rows),
        out_specs=(three, rows, rows),
        check_vma=False,
    )
```

```python
import functools

import jax
import jax.numpy as jnp
from jax import lax
from jax.experimental import pallas as pl
from jax.experimental.pallas import tpu as pltpu
from jax.sharding import PartitionSpec as P

HEADS = 12
HEAD = 128
FRAMES_GROUP = 3
WINDOW_FRAMES = 9
D = 1536
HALF = 768
BF = jnp.bfloat16
F32 = jnp.float32
MESH = pl.DeviceIdType.MESH


def rem(a, n):
    return lax.rem(a, jnp.int32(n))


def div(a, n):
    return lax.div(a, jnp.int32(n))


SCOPE = [None]


def sc(name=None):
    if SCOPE[0] is not None:
        SCOPE[0].__exit__(None, None, None)
    SCOPE[0] = None
    if name and PROFILE:
        SCOPE[0] = jax.named_scope(name)
        SCOPE[0].__enter__()


PROFILE = False
PRE = 2
MSG0 = (0, 2, 1)
MSG1 = ()


def owner(h):
    u, r = h // 3, h % 3
    zl = u // 2
    y = (u % 2) * 2 + (zl if r < 2 else 1 - zl)
    return zl * 8 + y * 2 + (r if r < 2 else 1)


def fused_kernel(
    stream_hbm, q_hbm, nk_hbm, nv_hbm, ck_hbm, cv_hbm, frames_hbm, group_hbm, step_hbm, gate_hbm, aow_hbm,
    cin_hbm, cot_hbm, w_hbm, so_ref, gin_hbm, gw_ref,
    stream_ref, frames_ref, group_ref, step_ref, gate_ref, w_ref,
    kbuf, vbuf, qbuf, aow, msg, got, ob, mixed,
    cin, cot, wown, tmp, wm, at, acc, dsend, drecv, rsend, rsend2,
    ra0, ra1, ra2, b0, b1, b2, b0s, b1s, b2s, rb0, rb1, rb2, fsend, frecv, obuf, gacc,
    ld_sem, p0_s, p0_r, g1_s, g1_r, g2_s, g2_r, push_s, push_r,
    d_s, d_r, a_s, a_r, b_s, b_r, f_s, f_r, o_sem, m_s, m_r, o_s, o_r,
):
    dp = lax.axis_index("dp")
    seq = lax.axis_index("seq")
    zh, x = div(dp, 4), rem(dp, 4)
    zl, y, c = div(seq, 8), div(rem(seq, 8), 2), rem(seq, 2)
    z = zh * 2 + zl
    xh, xl = div(x, 2), rem(x, 2)
    plane = y * 2 + c
    partner = (dp, seq + 1 - 2 * c)

    def xdev(xx):
        return (zh * 4 + xx, seq)

    def zdev(zz):
        return (div(zz, 2) * 4 + x, rem(zz, 2) * 8 + plane)

    def ydev(yy, cc):
        return (dp, zl * 8 + yy * 2 + cc)

    def rcopy(src, dst, s_sem, r_sem, dev):
        return pltpu.make_async_remote_copy(
            src_ref=src, dst_ref=dst, send_sem=s_sem, recv_sem=r_sem, device_id=dev, device_id_type=MESH
        )

    xs = [rem(x + s, 4) for s in (1, 2, 3)]
    ys = [rem(y + s, 4) for s in (1, 2, 3)]
    zs = [rem(z + s, 4) for s in (1, 2, 3)]
    plane_peers = [(rem(y + s, 4), c if k == 0 else 1 - c) for s in range(4) for k in range(2) if (s, k) != (0, 0)]
    others = [rem(seq + s, 16) for s in range(1, 16)]
    flat = [(rem(x + a, 4), rem(z + b, 4)) for a in range(4) for b in range(4) if (a, b) != (0, 0)]

    def xzdev(xx, zz):
        return (div(zz, 2) * 4 + xx, rem(zz, 2) * 8 + plane)


    sc("barrier")
    barrier = pltpu.get_barrier_semaphore()
    peers = [xdev(v) for v in xs] + [((1 - zh) * 4 + x, v * 8 + plane) for v in range(2)] + [(dp, v) for v in others]
    peers += [xzdev(a, b) for k, (a, b) in enumerate(flat) if (k + 1) // 4 and (k + 1) % 4]
    for dev in peers:
        pl.semaphore_signal(barrier, inc=1, device_id=dev, device_id_type=MESH)
    pairs = [(w_hbm, w_ref)]
    pairs += [(cot_hbm.at[:, pl.ds(h * HALF, HALF)], cot.at[h]) for h in range(2)]
    pairs += [(cin_hbm.at[:, pl.ds(t * 384, 384)], cin.at[t]) for t in range(4)]
    pairs += [(q_hbm, qbuf), (ck_hbm, kbuf.at[pl.ds(0, 96)]), (nk_hbm, kbuf.at[pl.ds(96, 32)]),
              (cv_hbm, vbuf.at[pl.ds(0, 96)]), (nv_hbm, vbuf.at[pl.ds(96, 32)]), (frames_hbm, frames_ref), (group_hbm, group_ref)]
    pairs += [(aow_hbm, aow), (stream_hbm, stream_ref), (gate_hbm, gate_ref), (step_hbm, step_ref)]
    loads = [pltpu.make_async_copy(a, b, ld_sem.at[k]) for k, (a, b) in enumerate(pairs)]
    for ld in loads:
        ld.start()

    p0 = [
        rcopy(wown.at[b], tmp.at[plane], p0_s.at[k], p0_r.at[k], ydev(a, b))
        for k, (a, b) in enumerate(plane_peers)
    ]

    def messages():
        for ld in loads[7:14]:
            ld.wait()
        first = FRAMES_GROUP * group_ref[0]
        frames = frames_ref[...]
        live = jnp.where((frames < first) & (frames >= first - WINDOW_FRAMES), 1.0, 0.0)
        live = jnp.broadcast_to(live, (16, 96)).astype(BF)
        for h in range(HEADS):
            cols = pl.ds(h * HEAD, HEAD)
            msg[h, pl.ds(0, 128), :] = kbuf[:, cols]
            msg[h, pl.ds(128, 128), :] = vbuf[:, cols]
            msg[h, pl.ds(256, 32), :] = qbuf[:, cols]
            msg[h, pl.ds(288, 16), :] = jnp.ones((16, HEAD), BF)
            msg[h, pl.ds(288, 16), pl.ds(0, 96)] = live

    def mcopy(h):
        return rcopy(msg.at[h], got.at[seq], m_s.at[h], m_r.at[seq], (dp, owner(h)))

    def send_messages(stage):
        for h in range(HEADS):
            same_z, same_y = zl == owner(h) // 8, y == owner(h) // 2 % 4
            if stage == 0:
                now = same_y & (seq != owner(h))
            elif stage == 1:
                now = same_z & jnp.logical_not(same_y)
            else:
                now = jnp.logical_not(same_z | same_y)

            @pl.when(now)
            def _():
                mcopy(h).start()

            if stage == 0:

                @pl.when(seq == owner(h))
                def _():
                    got[seq] = msg[h]

    def part2(ref, yy):
        return ref.at[..., pl.ds(pl.multiple_of(div(yy, 2) * 48, 48), 48), pl.ds(pl.multiple_of(512 + rem(yy, 2) * 128, 128), 128)]

    own = wm.at[c, zh, xh, xl, zl]
    g1 = []
    for k in range(3):
        g1.append(rcopy(own.at[:, pl.ds(0, 256)], own.at[:, pl.ds(0, 256)], g1_s.at[k], g1_r.at[k], xdev(xs[k])))
        g1.append(rcopy(own.at[:, pl.ds(256, 256)], own.at[:, pl.ds(256, 256)], g1_s.at[3 + k], g1_r.at[3 + k], zdev(zs[k])))
    for k, (a, b) in enumerate(flat):
        g1.append(rcopy(part2(own, y), part2(own, y), g1_s.at[6 + k], g1_r.at[6 + k], xzdev(a, b)))
    g2 = []
    w0 = wm.at[c, zh, :, :, zl, :, pl.ds(0, 256)]
    w1 = wm.at[c, :, xh, xl, :, :, pl.ds(256, 256)]
    w2 = part2(wm.at[c], y)
    for k in range(3):
        g2.append(rcopy(w0, w0, g2_s.at[k], g2_r.at[k], zdev(zs[k])))
        g2.append(rcopy(w1, w1, g2_s.at[3 + k], g2_r.at[3 + k], xdev(xs[k])))
        g2.append(rcopy(w2, w2, g2_s.at[6 + k], g2_r.at[6 + k], ydev(ys[k], c)))

    sc("ldwait")
    loads[0].wait()
    for h in range(2):
        wown[h] = jnp.zeros((16, HALF), BF)
        wown[h, pl.ds(0, 12), :] = w_ref[:, pl.ds(h * HALF, HALF)]
    for ld in loads[1:3]:
        ld.wait()
    sc()

    def dcopy(t):
        return rcopy(dsend.at[t], drecv.at[t], d_s.at[t], d_r.at[t], partner)

    def gw_tile(t):
        pltpu.make_async_copy(
            cin_hbm.at[:, pl.ds(pl.multiple_of(t * 384, 384), 384)], cin.at[t], ld_sem.at[3 + t]
        ).wait()
        at[...] = cin[t].T
        dsend[t] = lax.dot_general(
            at[...], cot[1 - c], (((1,), (0,)), ((), ())), preferred_element_type=F32
        ).astype(BF)
        acc[div(t, 2), rem(t, 2)] = lax.dot_general(
            at[...], cot[c], (((1,), (0,)), ((), ())), preferred_element_type=F32
        ).reshape(2, 2, 96, HALF)

    sc("gw0")

    @pl.loop(0, PRE)
    def _(t):
        gw_tile(t)

    sc("msg")
    messages()
    sc("barwait")
    pl.semaphore_wait(barrier, len(peers))
    for cp in p0:
        cp.start()
    tmp[plane] = wown[c]
    for t in range(PRE):
        dcopy(jnp.int32(t)).start()
    for k in MSG0:
        send_messages(k)
    sc("gw1")

    @pl.loop(PRE, 4)
    def _(t):
        gw_tile(t)
        dcopy(t).start()

    sc()

    sc("p0wait")
    for cp in p0:
        cp.wait_recv()
    row = lax.broadcasted_iota(jnp.int32, (96, 128), 0)
    col = lax.broadcasted_iota(jnp.int32, (96, 128), 1)
    pick = (col == div(row, 12) * 16 + rem(row, 12)).astype(BF)
    block = jnp.dot(pick, tmp[...].reshape(128, HALF), preferred_element_type=F32).astype(BF)
    own[:, pl.ds(0, 512)] = block[:, :512]
    for yy in range(4):
        i, j = yy // 2 * 48, 512 + yy % 2 * 128

        @pl.when(y == yy)
        def _():
            own[pl.ds(i, 48), pl.ds(j, 128)] = block[i : i + 48, j : j + 128]

    for cp in g1:
        cp.start()
    sc()

    @pl.loop(0, 4)
    def _(t):
        sc("dwait")
        dcopy(t).wait_recv()
        sc("chipsum")
        i, j = div(t, 2), rem(t, 2)
        both = acc[i, j] + drecv[t].reshape(2, 2, 96, HALF).astype(F32)
        acc[i, j] = both
        rsend[i, j] = both[..., :512].astype(BF)
        for yy in range(4):
            rsend2[yy, i, j] = both[:, :, (yy // 2) * 48 : (yy // 2) * 48 + 48, 512 + (yy % 2) * 128 : 640 + (yy % 2) * 128].astype(BF)
        sc()

    sc("rastart")
    ra = []
    for k in range(3):
        ra.append(rcopy(rsend.at[div(zs[k], 2), :, :, rem(zs[k], 2), :, pl.ds(0, 256)], ra0.at[k], a_s.at[k], a_r.at[k], zdev(zs[k])))
        ra.append(rcopy(rsend.at[:, div(xs[k], 2), rem(xs[k], 2), :, :, pl.ds(256, 256)], ra1.at[k], a_s.at[3 + k], a_r.at[3 + k], xdev(xs[k])))
        ra.append(rcopy(rsend2.at[ys[k]], ra2.at[k], a_s.at[6 + k], a_r.at[6 + k], ydev(ys[k], c)))
    for cp in ra:
        cp.start()
    for k in MSG1:
        send_messages(k)

    sc("g1wait")
    for cp in g1:
        cp.wait_recv()
    for cp in g2:
        cp.start()

    double = rem(y, 2) == zl
    active = double | (c == 1)
    head = 3 * (zl * 2 + div(y, 2)) + jnp.where(double, c, 2)

    def mixcopy(k):
        return rcopy(ob.at[others[k]], mixed.at[head], o_s.at[k], o_r.at[head], (dp, others[k]))

    sc("attwait")

    @pl.when(active)
    def _():
        for src in others:
            rcopy(msg.at[0], got.at[src], m_s.at[0], m_r.at[src], partner).wait_recv()

    sc("att")

    @pl.when(active)
    def _():
        alive = jnp.concatenate([got[j, pl.ds(288, 16), :] for j in range(16)], axis=1)[0:1].astype(F32) > 0.5

        @pl.loop(0, 4)
        def _(i):
            q = got[pl.ds(i * 4, 4), pl.ds(256, 32), :].reshape(128, HEAD)
            keys = got[:, pl.ds(0, 128), :].reshape(2048, HEAD)
            values = got[:, pl.ds(128, 128), :].reshape(2048, HEAD)
            scores = lax.dot_general(q, keys, (((1,), (1,)), ((), ())), preferred_element_type=F32) * (HEAD ** (-0.5))
            scores = jnp.where(alive, scores, -1e30)
            top = jnp.max(scores, axis=1, keepdims=True)
            weights = jnp.where(alive, jnp.exp(scores - top), 0.0)
            totals = jnp.sum(weights, axis=1, keepdims=True)
            summed = jnp.dot(weights.astype(BF), values, preferred_element_type=F32)
            ob[pl.ds(i * 4, 4)] = (summed / totals).astype(BF).reshape(4, 32, HEAD)

        for k in range(15):
            mixcopy(k).start()
        mixed[head] = ob[seq]

    sc("rawait")
    for cp in ra:
        cp.wait_recv()
    v0 = acc[zh, :, :, zl, :, 0:256]
    v1 = acc[:, xh, xl, :, :, 256:512]
    for k in range(3):
        v0 = v0 + ra0[k].astype(F32)
        v1 = v1 + ra1[k].astype(F32)
    b0[...] = v0
    b1[...] = v1
    b0s[...] = v0.astype(BF)
    b1s[...] = v1.astype(BF)
    v2 = rsend2[y].astype(F32)
    for k in range(3):
        v2 = v2 + ra2[k].astype(F32)
    b2[...] = v2
    b2s[...] = v2.astype(BF)
    rb = []
    for k in range(3):
        rb.append(rcopy(b0s.at[div(xs[k], 2), rem(xs[k], 2)], rb0.at[k], b_s.at[k], b_r.at[k], xdev(xs[k])))
        rb.append(rcopy(b1s.at[div(zs[k], 2), rem(zs[k], 2)], rb1.at[k], b_s.at[3 + k], b_r.at[3 + k], zdev(zs[k])))
    for k, (a, b) in enumerate(flat):
        src = b2s.at[div(b, 2), div(a, 2), rem(a, 2), rem(b, 2)]
        rb.append(rcopy(src, rb2.at[k], b_s.at[6 + k], b_r.at[6 + k], xzdev(a, b)))

    for cp in rb:
        cp.start()
    def pcopy(k, t):
        src = wm.at[c, div(t, 2), rem(t, 2), :, :, :, pl.ds(256 - 256 * k, 512 - 256 * k)]
        return rcopy(src, src, push_s.at[4 * k + t], push_r.at[4 * k + t], partner)

    sc("g2wait")
    for cp in g2[1::3] + g2[2::3]:
        cp.wait_recv()
    for t in range(4):
        pcopy(0, jnp.int32(t)).start()
    sc()

    def ocopy(t):
        return pltpu.make_async_copy(obuf.at[t], gin_hbm.at[:, pl.ds(pl.multiple_of(t * 384, 384), 384)], o_sem.at[t])

    def gin_part(t, lo, width):
        i, j = div(t, 2), rem(t, 2)
        dims = (((1,), (1,)), ((), ()))
        cols = pl.ds(lo, width)
        res = lax.dot_general(cot[0, :, cols], wm[0, i, j, :, :, :, cols].reshape(384, width), dims, preferred_element_type=F32)
        return res + lax.dot_general(cot[1, :, cols], wm[1, i, j, :, :, :, cols].reshape(384, width), dims, preferred_element_type=F32)

    @pl.loop(0, 4)
    def _(t):
        sc("pwait")
        pcopy(0, t).wait_recv()
        sc("gin")
        gacc[t] = gin_part(t, 256, 512)
        sc()

    sc("rbwait2")
    for cp in rb:
        cp.wait_recv()
    r0 = b0[xh, xl]
    r1 = b1[zh, zl]
    for k in range(3):
        r0 = r0 + rb0[k].astype(F32)
        r1 = r1 + rb1[k].astype(F32)
    sc("last")
    r2 = b2[zh, xh, xl, zl]
    for k in range(15):
        r2 = r2 + rb2[k].astype(F32)

    row = lax.broadcasted_iota(jnp.int32, (96, 256), 0)
    col = lax.broadcasted_iota(jnp.int32, (96, 256), 1)
    mine = (div(row, 48) == div(y, 2)) & (div(col, 128) == rem(y, 2))
    r2 = jnp.concatenate([r2, r2], axis=0)
    r2 = jnp.where(mine, jnp.concatenate([r2, r2], axis=1), 0.0)
    row = lax.broadcasted_iota(jnp.int32, (128, 96), 0)
    col = lax.broadcasted_iota(jnp.int32, (128, 96), 1)
    place = ((col == div(row, 16) * 12 + rem(row, 16)) & (rem(row, 16) < 12)).astype(BF)
    full = jnp.concatenate([r0, r1, r2], axis=1).astype(BF)
    fsend[...] = jnp.dot(place, full, preferred_element_type=F32).astype(BF).reshape(8, 16, HALF)
    fin = [
        rcopy(fsend.at[a * 2 + b], frecv.at[plane], f_s.at[k], f_r.at[k], ydev(a, b))
        for k, (a, b) in enumerate(plane_peers)
    ]
    for cp in fin:
        cp.start()
    frecv[plane] = fsend[plane]

    sc("g2wait2")
    for cp in g2[0::3]:
        cp.wait_recv()
    for t in range(4):
        pcopy(1, jnp.int32(t)).start()

    sc("mixwait")
    for h in range(HEADS):

        @pl.when(seq != owner(h))
        def _():
            rcopy(ob.at[0], mixed.at[h], o_s.at[0], o_r.at[h], partner).wait_recv()

    for ld in loads[14:]:
        ld.wait()
    sc("proj")
    joined = jnp.concatenate([mixed[h] for h in range(HEADS)], axis=1)
    projected = jnp.dot(joined, aow[...], preferred_element_type=F32)
    row = lax.broadcasted_iota(jnp.int32, (4, D), 0)
    gate = jnp.sum(jnp.where(row == step_ref[0], gate_ref[...], 0.0), axis=0, keepdims=True)
    so_ref[...] = (stream_ref[...].astype(F32) + gate * projected).astype(BF)

    sc()

    @pl.loop(0, 4)
    def _(t):
        sc("pwait")
        pcopy(1, t).wait_recv()
        sc("gin")
        obuf[t] = (gacc[t] + gin_part(t, 0, 256)).astype(BF)
        ocopy(t).start()
        sc()

    sc("finwait")
    for cp in fin:
        cp.wait_recv()
    sc("drain")
    factor = float(131072) ** (-0.5)
    for h in range(2):
        total = frecv[h].astype(F32)
        for yy in range(1, 4):
            total = total + frecv[yy * 2 + h].astype(F32)
        gw_ref[:, pl.ds(h * HALF, HALF)] = total[:12] * factor

    for cp in p0 + g1 + g2 + ra + rb + fin:
        cp.wait_send()
    for t in range(4):
        dcopy(jnp.int32(t)).wait_send()
        pcopy(0, jnp.int32(t)).wait_send()
        pcopy(1, jnp.int32(t)).wait_send()
        ocopy(jnp.int32(t)).wait()
    for h in range(HEADS):

        @pl.when(seq != owner(h))
        def _():
            mcopy(h).wait_send()

    @pl.when(active)
    def _():
        for k in range(15):
            mixcopy(k).wait_send()

    sc()


def local(stream, queries, new_keys, new_values, cache_keys, cache_values, cache_frames, group_index, timestep, gate_table, attn_out_weight, critic_in, critic_cot, critic_weight):
    dma = pltpu.SemaphoreType.DMA
    V = pltpu.VMEM
    anywhere = pl.BlockSpec(memory_space=pl.ANY)
    vmem = pl.BlockSpec(memory_space=pltpu.VMEM)
    so, gin, gw = pl.pallas_call(
        fused_kernel,
        out_shape=(
            jax.ShapeDtypeStruct((32, D), BF),
            jax.ShapeDtypeStruct((1024, D), BF),
            jax.ShapeDtypeStruct((12, D), F32),
        ),
        in_specs=[anywhere] * 14,
        out_specs=(vmem, anywhere, vmem),
        scratch_shapes=[
            V((32, D), BF), V((1, 96), jnp.int32), pltpu.SMEM((1,), jnp.int32), pltpu.SMEM((1,), jnp.int32), V((4, D), F32), V((12, D), BF),
            V((128, D), BF), V((128, D), BF), V((32, D), BF), V((D, D), BF), V((HEADS, 304, HEAD), BF),
            V((16, 304, HEAD), BF), V((16, 32, HEAD), BF), V((HEADS, 32, HEAD), BF),
            V((4, 1024, 384), BF), V((2, 1024, HALF), BF), V((2, 16, HALF), BF), V((8, 16, HALF), BF),
            V((2, 2, 2, 2, 2, 96, HALF), BF), V((384, 1024), BF), V((2, 2, 2, 2, 96, HALF), F32),
            V((4, 384, HALF), BF), V((4, 384, HALF), BF),
            V((2, 2, 2, 2, 96, 512), BF), V((4, 2, 2, 2, 2, 48, 128), BF),
            V((3, 2, 2, 96, 256), BF), V((3, 2, 2, 96, 256), BF), V((3, 2, 2, 2, 2, 48, 128), BF),
            V((2, 2, 96, 256), F32), V((2, 2, 96, 256), F32), V((2, 2, 2, 2, 48, 128), F32),
            V((2, 2, 96, 256), BF), V((2, 2, 96, 256), BF), V((2, 2, 2, 2, 48, 128), BF),
            V((3, 96, 256), BF), V((3, 96, 256), BF), V((15, 48, 128), BF),
            V((8, 16, HALF), BF), V((8, 16, HALF), BF), V((4, 1024, 384), BF), V((4, 1024, 384), F32),
            dma((18,)), dma((7,)), dma((7,)), dma((21,)), dma((21,)), dma((9,)), dma((9,)),
            dma((8,)), dma((8,)), dma((4,)), dma((4,)), dma((9,)), dma((9,)), dma((21,)), dma((21,)),
            dma((7,)), dma((7,)), dma((4,)), dma((12,)), dma((16,)), dma((15,)), dma((12,)),
        ],
        compiler_params=pltpu.CompilerParams(
            collective_id=0, has_side_effects=True, vmem_limit_bytes=60 * 1024 * 1024
        ),
        cost_estimate=pl.CostEstimate(flops=10500000000, bytes_accessed=25000000, transcendentals=1000000),
    )(
        stream[0], queries[0], new_keys[0], new_values[0], cache_keys[0], cache_values[0], cache_frames,
        group_index, timestep, gate_table, attn_out_weight, critic_in, critic_cot, critic_weight,
    )
    return (so[None], gin, gw)


def solution(mesh):
    three = P("dp", "seq", None)
    rows = P(("dp", "seq"), None)
    return jax.shard_map(
        local,
        mesh=mesh,
        in_specs=(three,) * 6 + (P("dp", "seq"), P("dp"), P("dp"), P(), P(), rows, rows, rows),
        out_specs=(three, rows, rows),
        check_vma=False,
    )
```
